32 devices in a mesh: data: 2 (over x), ys: 4 (over z), xs: 4 (over y, core).
Axes of the slice: x: 2, y: 2, z: 4, core: 2. Of those that a mesh axis runs over, the one named last changes fastest.
Arguments:
- field: float32 [128, 32, 32, 32, 32], P('data', 'xs', 'ys'), parts along dimension 0
- spec_real: float32 [2, 16, 16, 8, 32, 32], replicated
- spec_imag: float32 [2, 16, 16, 8, 32, 32], replicated
- mix_weight: float32 [2, 32, 32], replicated
- bias: float32 [2, 32], replicated
Outputs:
- output: float32 [128, 32, 32, 32, 32], P('data', 'xs', 'ys'), parts along dimension 0
There are 2 independent parts. The reference program is written for one: setup_inputs(seed, part) draws one part's arguments, and reference() takes and returns one part's arrays. A program takes and returns all parts, laid end to end along the dimension named above; an argument that names none is the same for every part.
All inputs are finite; a program needn't handle non-finite values.
Results may differ from the reference program's by a relative error of at most 0.001.
Values are sent between devices in bfloat16 or wider.
A program may use at most 1 GiB of HBM per device.

```python
import jax
import jax.numpy as jnp
from jax import lax

PART_BATCH = 64
GRID_X = 32
GRID_Y = 32
GRID_Z = 32
WIDTH = 32
MODES = 8
LAYERS = 2


def spread_modes(kept, first):
    dims = kept.shape
    gap_x = dims[:first] + (GRID_X - 2 * MODES,) + dims[first + 1:]
    full_x = jnp.concatenate([lax.slice_in_dim(kept, 0, MODES, axis=first), jnp.zeros(gap_x, kept.dtype), lax.slice_in_dim(kept, MODES, 2 * MODES, axis=first)], axis=first)
    dims = full_x.shape
    gap_y = dims[:first + 1] + (GRID_Y - 2 * MODES,) + dims[first + 2:]
    full_y = jnp.concatenate([lax.slice_in_dim(full_x, 0, MODES, axis=first + 1), jnp.zeros(gap_y, kept.dtype), lax.slice_in_dim(full_x, MODES, 2 * MODES, axis=first + 1)], axis=first + 1)
    dims = full_y.shape
    gap_z = dims[:first + 2] + (GRID_Z // 2 + 1 - MODES,) + dims[first + 3:]
    return jnp.concatenate([full_y, jnp.zeros(gap_z, kept.dtype)], axis=first + 2)


def setup_inputs(seed: int = 0, part: int = 0) -> dict:
    part_keys = jax.random.split(jax.random.fold_in(jax.random.key(seed), part), 3)
    shared_keys = jax.random.split(jax.random.key(seed + 1), 4)
    kept_shape = (PART_BATCH, 2 * MODES, 2 * MODES, MODES, WIDTH)
    coef_scale = 0.25 * MODES ** -1.5
    kept = lax.complex(jax.random.normal(part_keys[0], kept_shape, jnp.float32), jax.random.normal(part_keys[1], kept_shape, jnp.float32)) * coef_scale
    smooth = jnp.fft.irfftn(spread_modes(kept, 1), s=(GRID_X, GRID_Y, GRID_Z), axes=(1, 2, 3), norm='forward')
    noise = 0.3 * jax.random.normal(part_keys[2], (PART_BATCH, GRID_X, GRID_Y, GRID_Z, WIDTH), jnp.float32)
    kernel_shape = (LAYERS, 2 * MODES, 2 * MODES, MODES, WIDTH, WIDTH)
    kernel_scale = (2.0 * WIDTH) ** -0.5
    return dict(
        field=smooth + noise,
        spec_real=kernel_scale * jax.random.normal(shared_keys[0], kernel_shape, jnp.float32),
        spec_imag=kernel_scale * jax.random.normal(shared_keys[1], kernel_shape, jnp.float32),
        mix_weight=WIDTH ** -0.5 * jax.random.normal(shared_keys[2], (LAYERS, WIDTH, WIDTH), jnp.float32),
        bias=0.5 * jax.random.normal(shared_keys[3], (LAYERS, WIDTH), jnp.float32),
    )


def spectral_conv(sample, kernel):
    spec = jnp.fft.rfftn(sample, axes=(0, 1, 2))
    kept_x = jnp.concatenate([spec[:MODES], spec[GRID_X - MODES:]], axis=0)
    kept = jnp.concatenate([kept_x[:, :MODES], kept_x[:, GRID_Y - MODES:]], axis=1)[:, :, :MODES]
    mixed = jnp.einsum('abci,abcio->abco', kept, kernel)
    return jnp.fft.irfftn(spread_modes(mixed, 0), s=(GRID_X, GRID_Y, GRID_Z), axes=(0, 1, 2))


def reference(field, spec_real, spec_imag, mix_weight, bias):
    def layer_step(carry, weights):
        real_part, imag_part, w_mix, b_vec = weights
        kernel = lax.complex(real_part, imag_part)
        spectral = lax.map(lambda sample: spectral_conv(sample, kernel), carry)
        pointwise = jnp.dot(carry, w_mix, preferred_element_type=jnp.float32)
        return jax.nn.gelu(spectral + pointwise + b_vec, approximate=True), None

    final_field, unused = lax.scan(layer_step, field, (spec_real, spec_imag, mix_weight, bias))
    return final_field
```

```python
import functools
import math
import jax
import jax.numpy as jnp
from jax import lax
from jax.experimental import pallas as pl
from jax.experimental.pallas import tpu as pltpu
from jax.sharding import PartitionSpec as P

EXACT = lax.Precision.HIGHEST
HALF = 64
SUB = 8
ROOT_HALF = math.sqrt(0.5)


def turn(value, cosine, sine):
    re, im = value
    near = lambda a, b: abs(a - b) < 1e-12
    if near(cosine, 1.0):
        return re, im
    if near(cosine, -1.0):
        return -re, -im
    if near(sine, 1.0):
        return -im, re
    if near(sine, -1.0):
        return im, -re
    if near(abs(cosine), abs(sine)):
        a = re if cosine > 0 else -re
        b = im if cosine > 0 else -im
        same = (cosine > 0) == (sine > 0)
        if same:
            return (a - b) * abs(cosine), (a + b) * abs(cosine)
        return (a + b) * abs(cosine), (b - a) * abs(cosine)
    return re * cosine - im * sine, re * sine + im * cosine


def add(a, b):
    return a[0] + b[0], a[1] + b[1]


def sub(a, b):
    return a[0] - b[0], a[1] - b[1]


def fft(values, sign):
    size = len(values)
    if size == 1:
        return values
    even = fft(values[0::2], sign)
    odd = fft(values[1::2], sign)
    low, high = [], []
    for k in range(size // 2):
        angle = sign * 2.0 * math.pi * k / size
        twisted = turn(odd[k], math.cos(angle), math.sin(angle))
        low.append(add(even[k], twisted))
        high.append(sub(even[k], twisted))
    return low + high


def real_forward(tiles):
    size = len(tiles)
    half = size // 2
    packed = fft([(tiles[2 * j], tiles[2 * j + 1]) for j in range(half)], -1.0)
    first = packed[0]
    out = [(first[0] + first[1], jnp.zeros_like(first[0]))]
    for k in range(1, size // 4):
        a, b = packed[k], packed[half - k]
        even = ((a[0] + b[0]) * 0.5, (a[1] - b[1]) * 0.5)
        odd = ((a[1] + b[1]) * 0.5, (b[0] - a[0]) * 0.5)
        angle = -2.0 * math.pi * k / size
        out.append(add(even, turn(odd, math.cos(angle), math.sin(angle))))
    return out


def real_inverse(kept, scale):
    count = len(kept)
    half = 2 * count
    size = 2 * half
    packed = [None] * half
    head = kept[0][0] * scale
    packed[0] = (head, head)
    packed[count] = (jnp.zeros_like(head), jnp.zeros_like(head))
    for k in range(1, count):
        re, im = kept[k]
        angle = 2.0 * math.pi * k / size
        c, s = math.cos(angle), math.sin(angle)
        packed[k] = turn((re, im), (1.0 - s) * scale, c * scale)
        packed[half - k] = turn((re, -im), (1.0 + s) * scale, c * scale)
    out = []
    for pair in fft(packed, 1.0):
        out.extend(pair)
    return out


def freq(q, kept, size):
    return q if q < kept // 2 else q + size - kept


def join(a, b):
    return jnp.concatenate([a, b], axis=-1)


def gelu(x):
    inner = (x + 0.044715 * x * x * x) * math.sqrt(2.0 / math.pi)
    return 0.5 * x * (1.0 + jnp.tanh(inner))


def slot(owner, me, devs):
    return lax.rem(owner - me + devs, devs)


def put_modes(kept, outs, at, held, me):
    devs = len(outs[0])
    for k, (re, im) in enumerate(kept):
        r = slot(k // 2, me, devs)
        held[r, k % 2, 0] = re
        held[r, k % 2, 1] = im
    for kk in range(2):
        for r in range(devs):
            for p in range(2):
                outs[kk][r][p, 0, 0, at, :] = held[r, kk, p]


def loop_tiles(width, body):
    @pl.loop(0, width // SUB)
    def _(t):
        body(pl.ds(pl.multiple_of(t * SUB, SUB), SUB))


def first_kernel(devs, pos_ref, v_ref, pair_ref, *rest):
    outs, held = (rest[:devs], rest[devs:2 * devs]), rest[-1]
    depth, width = v_ref.shape[2], v_ref.shape[3]

    def body(at):
        tiles = []
        for z in range(depth):
            tile = join(v_ref[0, 0, z, at, :], v_ref[0, 1, z, at, :])
            pair_ref[0, 0, z, at, :] = tile
            tiles.append(tile)
        put_modes(real_forward(tiles), outs, at, held, pos_ref[1])

    loop_tiles(width, body)


def point_kernel(v_ref, w_ref, b_ref, o_ref):
    depth = v_ref.shape[2]
    group = 8

    @pl.loop(0, depth // group)
    def _(g):
        cols = jnp.concatenate([v_ref[0, 0, g * group + i] for i in range(group)], axis=-1)
        out = jnp.dot(w_ref[...], cols, precision=EXACT, preferred_element_type=jnp.float32)
        for i in range(group):
            o_ref[0, 0, g * group + i] = out[:, i * 2 * HALF:(i + 1) * 2 * HALF] + b_ref[...]


def forward_x_kernel(x_devs, pos_ref, *refs):
    ins, held = refs[:x_devs], refs[-1]
    outs = refs[x_devs:-1]
    _, x_loc, _, width, _ = ins[0].shape
    size = x_devs * x_loc
    kept = size // 2
    devs, per = len(outs), outs[0].shape[0]

    def load(x):
        ref = ins[(x_devs - x // x_loc) % x_devs]
        return lambda at: (ref[0, x % x_loc, 0, at, :], ref[1, x % x_loc, 0, at, :])

    def body(at):
        even = fft([load(x)(at) for x in range(0, size, 2)], -1.0)
        odd = fft([load(x)(at) for x in range(1, size, 2)], -1.0)
        for q in range(kept):
            angle = -2.0 * math.pi * freq(q, kept, size) / size
            re, im = add(even[q], turn(odd[q], math.cos(angle), math.sin(angle)))
            r = slot(q // per, pos_ref[0], devs)
            held[r, q % per, 0] = re
            held[r, q % per, 1] = im
        for r in range(devs):
            for i in range(per):
                for p in range(2):
                    outs[r][i, p, 0, at, :] = held[r, i, p]

    loop_tiles(width, body)


def inverse_x_kernel(devs, pos_ref, *refs):
    ins, held = refs[:devs], refs[-1]
    outs = refs[devs:-1]
    per = ins[0].shape[0]
    _, x_loc, _, width, _ = outs[0].shape
    size = len(outs) * x_loc
    kept = size // 2

    def body(at):
        for r in range(devs):
            owner = slot(pos_ref[0], r, devs)
            for i in range(per):
                for p in range(2):
                    held[owner, i, p] = ins[r][i, p, 0, at, :]
        modes = [(held[q // per, q % per, 0], held[q // per, q % per, 1]) for q in range(kept)]
        for odd in range(2):
            twisted = []
            for q in range(kept):
                angle = 2.0 * math.pi * odd * freq(q, kept, size) / size
                twisted.append(turn(modes[q], math.cos(angle), math.sin(angle)))
            for i, (re, im) in enumerate(fft(twisted, 1.0)):
                x = 2 * i + odd
                outs[x // x_loc][0, x % x_loc, 0, at, :] = re
                outs[x // x_loc][1, x % x_loc, 0, at, :] = im

    loop_tiles(width, body)


def mix_kernel(devs, parts, pos_ref, *refs):
    count = devs * parts
    ins, (re_ref, im_ref), outs = refs[:count], refs[count:count + 2], refs[count + 2:2 * count + 2]
    spec_ref, mixed_ref = refs[2 * count + 2:]
    _, _, part, width, lanes = ins[0].shape
    kept = count * part
    size = 2 * kept
    low = lax.broadcasted_iota(jnp.int32, (SUB, lanes), 1) < HALF
    low_wide = lax.broadcasted_iota(jnp.int32, (width, lanes), 1) < HALF

    def place(j):
        ahead, pair = divmod(j, parts * part)
        return ahead, pair // part, pair % part

    def forward(at):
        values = []
        for j in range(kept):
            ahead, h, i = place(j)
            ref = ins[h * devs + (devs - ahead) % devs]
            values.append((ref[0, 0, i, at, :], ref[0, 1, i, at, :]))
        modes = fft(values, -1.0)
        for q in range(kept):
            angle = -2.0 * math.pi * freq(q, kept, size) / size
            re, im = modes[q]
            far_re, far_im = turn((re, im), math.cos(angle), math.sin(angle))
            near = jnp.where(low, re, far_im)
            far = jnp.where(low, im, far_re)
            spec_ref[q, at, :] = near + pltpu.roll(far, HALF, 1)

    loop_tiles(width, forward)
    flip = jnp.where(low_wide, -1.0, 1.0)
    for q in range(kept):
        weight = jnp.concatenate([re_ref[0, 0, q, 0], im_ref[0, 0, q, 0]], axis=-1)
        out = lax.dot_general(weight, spec_ref[q], (((0,), (0,)), ((), ())), precision=EXACT, preferred_element_type=jnp.float32)
        mixed_ref[q] = out[:width] + pltpu.roll(out[width:], HALF, 1) * flip

    def inverse(at):
        twisted = []
        for q in range(kept):
            both = mixed_ref[q, at, :]
            swap = pltpu.roll(both, HALF, 1)
            re, im = jnp.where(low, both, swap), jnp.where(low, swap, both)
            angle = 2.0 * math.pi * freq(q, kept, size) / size
            far_re, far_im = turn((re, im), math.cos(angle), math.sin(angle))
            twisted.append((jnp.where(low, re, far_re), jnp.where(low, im, far_im)))
        for j, (re, im) in enumerate(fft(twisted, 1.0)):
            ahead, h, i = place(j)
            outs[h * devs + ahead][0, 0, i, at, :] = re
            outs[h * devs + ahead][0, 1, i, at, :] = im

    loop_tiles(width, inverse)


def last_kernel(devs, scale, more, pos_ref, *refs):
    ins, p_ref, rest = (refs[:devs], refs[devs:2 * devs]), refs[2 * devs], refs[2 * devs + 1:]
    got, held = rest[-2:]
    depth, width = p_ref.shape[2], p_ref.shape[3]
    me = pos_ref[1]

    def body(at):
        for r in range(devs):
            owner = slot(me, r, devs)
            for kk in range(2):
                for p in range(2):
                    got[owner, kk, p] = ins[kk][r][p, 0, 0, at, :]
        spectral = real_inverse([(got[k // 2, k % 2, 0], got[k // 2, k % 2, 1]) for k in range(2 * devs)], scale)
        fresh = []
        for z in range(depth):
            tile = gelu(spectral[z] + p_ref[0, 0, z, at, :])
            if more:
                rest[0][0, 0, z, at, :] = tile
                fresh.append(tile)
            else:
                rest[-3][0, 0, z, at, :] = tile[:, :HALF]
                rest[-3][0, 1, z, at, :] = tile[:, HALF:]
        if more:
            put_modes(real_forward(fresh), (rest[1:devs + 1], rest[devs + 1:2 * devs + 1]), at, held, me)

    loop_tiles(width, body)


PARTS = 2


def cost(us):
    return pl.CostEstimate(flops=int(us * FLOPS_PER_US), bytes_accessed=1048576, transcendentals=0)


FLOPS_PER_US = 30000000


def solution(mesh):
    row_devs = mesh.shape['ys']
    col_devs = mesh.shape['xs']

    def local_layers(field, spec_real, spec_imag, mix_weight, bias):
        batch, x_loc, y_loc, grid_z, width = field.shape
        modes = spec_real.shape[3]
        layers = spec_real.shape[0]
        lanes = 2 * batch
        pairs = y_loc // 2
        part = pairs // PARTS
        per = 2 * modes // row_devs
        scale = 1.0 / (x_loc * col_devs * y_loc * row_devs * grid_z)
        shape = lambda *dims: jax.ShapeDtypeStruct(dims, jnp.float32)
        scratch = lambda *dims: pltpu.VMEM(dims, jnp.float32)
        wave = (2, x_loc, part, width, lanes)
        freqs = (per, 2, part, width, lanes)
        cells = (x_loc, part, grid_z, width, lanes)
        wave_cell = pl.BlockSpec((2, 1, 1, width, lanes), lambda x, y, pos: (0, x, y, 0, 0))
        wave_row = pl.BlockSpec((2, x_loc, 1, width, lanes), lambda y, pos: (0, 0, y, 0, 0))
        freq_row = pl.BlockSpec((per, 2, 1, width, lanes), lambda y, pos: (0, 0, y, 0, 0))
        freq_cell = pl.BlockSpec((1, 2, part, width, lanes), lambda q, pos: (q, 0, 0, 0, 0))
        cell = pl.BlockSpec((1, 1, grid_z, width, lanes), lambda x, y, pos: (x, y, 0, 0, 0))
        loose = lambda h: pl.BlockSpec((1, 2, grid_z, width, batch), lambda x, y, pos: (x, y + h * part, 0, 0, 0))
        position = jnp.stack([lax.axis_index('ys'), lax.axis_index('xs')]).astype(jnp.int32)

        def call(body, name, us, grid, ins, outs, shapes, scratches, *operands, alias=None):
            spec = pltpu.PrefetchScalarGridSpec(num_scalar_prefetch=1, grid=grid, in_specs=ins, out_specs=outs, scratch_shapes=scratches)
            return pl.pallas_call(body, grid_spec=spec, out_shape=shapes, name=name, cost_estimate=cost(us), input_output_aliases=alias or {},
                                  compiler_params=pltpu.CompilerParams(dimension_semantics=('arbitrary',) * len(grid)))(position, *operands)

        def swap(arrays, axis):
            devs = len(arrays)
            return [arrays[0]] + [lax.ppermute(arrays[r], axis, [(i, (i + r) % devs) for i in range(devs)]) for r in range(1, devs)]

        def first(h, grid_field):
            out = call(functools.partial(first_kernel, col_devs), 'first', 18, (x_loc, part), [loose(h)], [cell] + [wave_cell] * (2 * col_devs),
                       [shape(*cells)] + [shape(*wave)] * (2 * col_devs), [scratch(col_devs, 2, 2, SUB, lanes)], grid_field)
            return out[0], [out[1:1 + col_devs], out[1 + col_devs:]]

        def forward_x(arrays):
            return call(functools.partial(forward_x_kernel, col_devs), 'forward_x', 3, (part,), [wave_row] * col_devs, [freq_row] * row_devs,
                        [shape(*freqs)] * row_devs, [scratch(row_devs, per, 2, SUB, lanes)], *arrays)

        def inverse_x(arrays):
            return call(functools.partial(inverse_x_kernel, row_devs), 'inverse_x', 3, (part,), [freq_row] * row_devs, [wave_row] * col_devs,
                        [shape(*wave)] * col_devs, [scratch(row_devs, per, 2, SUB, lanes)], *arrays)

        def mix(layer, kk, arrays):
            weight = pl.BlockSpec((1, 1, 2 * modes, 1, width, width), lambda q, pos: (layer, pos[0] * per + q, 0, 2 * pos[1] + kk, 0, 0))
            count = row_devs * PARTS
            out = call(functools.partial(mix_kernel, row_devs, PARTS), 'mix', 11, (per,), [freq_cell] * count + [weight] * 2, [freq_cell] * count,
                       [shape(*freqs)] * count, [scratch(2 * modes, width, lanes)] * 2, *arrays, spec_real, spec_imag)
            return [out[h * row_devs:(h + 1) * row_devs] for h in range(PARTS)]

        def point(layer, value):
            body = lambda pos_ref, *refs: point_kernel(*refs)
            whole = lambda *dims: pl.BlockSpec(dims, lambda x, y, pos: (0, 0))
            return call(body, 'point', 19, (x_loc, part), [cell, whole(width, width), whole(width, lanes)], cell, shape(*cells), [],
                        value, mix_weight[layer].T, jnp.broadcast_to(bias[layer][:, None], (width, lanes)))

        def last(h, more, arrays, local, target):
            scratches = [scratch(col_devs, 2, 2, SUB, lanes)] * 2
            body = functools.partial(last_kernel, col_devs, scale, more)
            ins = [wave_cell] * (2 * col_devs) + [cell]
            if more:
                out = call(body, 'last', 17, (x_loc, part), ins, [cell] + [wave_cell] * (2 * col_devs), [shape(*cells)] + [shape(*wave)] * (2 * col_devs), scratches, *arrays, local)
                return out[0], [out[1:1 + col_devs], out[1 + col_devs:]]
            whole = shape(x_loc, y_loc, grid_z, width, batch)
            if target is None:
                return call(body, 'last', 18, (x_loc, part), ins, loose(h), whole, scratches, *arrays, local)
            return call(body, 'last', 18, (x_loc, part), ins + [pl.BlockSpec(memory_space=pl.ANY)], loose(h), whole, scratches, *arrays, local, target, alias={len(ins) + 1: 0})

        grid_field = field.transpose(1, 2, 3, 4, 0)
        values, waves = zip(*[first(h, grid_field) for h in range(PARTS)])
        target = None
        for layer in range(layers):
            locals_ = [point(layer, v) for v in values]
            here = [[swap(waves[h][kk], 'xs') for h in range(PARTS)] for kk in range(2)]
            along = [[swap(forward_x(here[kk][h]), 'ys') for h in range(PARTS)] for kk in range(2)]
            mixed = [mix(layer, kk, along[kk][0] + along[kk][1]) for kk in range(2)]
            back = [[swap(inverse_x(swap(mixed[kk][h], 'ys')), 'xs') for h in range(PARTS)] for kk in range(2)]
            more = layer + 1 < layers
            if more:
                values, waves = zip(*[last(h, True, list(back[0][h]) + list(back[1][h]), locals_[h], None) for h in range(PARTS)])
            else:
                for h in range(PARTS):
                    target = last(h, False, list(back[0][h]) + list(back[1][h]), locals_[h], target)
        return target.transpose(4, 0, 1, 2, 3)

    field_spec = P('data', 'xs', 'ys', None, None)
    return jax.shard_map(local_layers, mesh=mesh, in_specs=(field_spec, P(), P(), P(), P()), out_specs=field_spec, check_vma=False)
```

```python
import functools
import math
import jax
import jax.numpy as jnp
from jax import lax
from jax.experimental import pallas as pl
from jax.experimental.pallas import tpu as pltpu
from jax.sharding import PartitionSpec as P

EXACT = lax.Precision.HIGHEST
HALF = 64
SUB = 8


def turn(value, cosine, sine):
    re, im = value
    near = lambda a, b: abs(a - b) < 1e-12
    if near(cosine, 1.0):
        return re, im
    if near(cosine, -1.0):
        return -re, -im
    if near(sine, 1.0):
        return -im, re
    if near(sine, -1.0):
        return im, -re
    if near(abs(cosine), abs(sine)):
        a = re if cosine > 0 else -re
        b = im if cosine > 0 else -im
        same = (cosine > 0) == (sine > 0)
        if same:
            return (a - b) * abs(cosine), (a + b) * abs(cosine)
        return (a + b) * abs(cosine), (b - a) * abs(cosine)
    return re * cosine - im * sine, re * sine + im * cosine


def add(a, b):
    return a[0] + b[0], a[1] + b[1]


def sub(a, b):
    return a[0] - b[0], a[1] - b[1]


def fft(values, sign):
    size = len(values)
    if size == 1:
        return values
    even = fft(values[0::2], sign)
    odd = fft(values[1::2], sign)
    low, high = [], []
    for k in range(size // 2):
        angle = sign * 2.0 * math.pi * k / size
        twisted = turn(odd[k], math.cos(angle), math.sin(angle))
        low.append(add(even[k], twisted))
        high.append(sub(even[k], twisted))
    return low + high


def real_forward(tiles):
    size = len(tiles)
    half = size // 2
    packed = fft([(tiles[2 * j], tiles[2 * j + 1]) for j in range(half)], -1.0)
    first = packed[0]
    out = [(first[0] + first[1], jnp.zeros_like(first[0]))]
    for k in range(1, size // 4):
        a, b = packed[k], packed[half - k]
        even = ((a[0] + b[0]) * 0.5, (a[1] - b[1]) * 0.5)
        odd = ((a[1] + b[1]) * 0.5, (b[0] - a[0]) * 0.5)
        angle = -2.0 * math.pi * k / size
        out.append(add(even, turn(odd, math.cos(angle), math.sin(angle))))
    return out


def real_inverse(kept, scale):
    count = len(kept)
    half = 2 * count
    size = 2 * half
    packed = [None] * half
    head = kept[0][0] * scale
    packed[0] = (head, head)
    packed[count] = (jnp.zeros_like(head), jnp.zeros_like(head))
    for k in range(1, count):
        re, im = kept[k]
        angle = 2.0 * math.pi * k / size
        c, s = math.cos(angle), math.sin(angle)
        packed[k] = turn((re, im), (1.0 - s) * scale, c * scale)
        packed[half - k] = turn((re, -im), (1.0 + s) * scale, c * scale)
    out = []
    for pair in fft(packed, 1.0):
        out.extend(pair)
    return out


def freq(q, kept, size):
    return q if q < kept // 2 else q + size - kept


def join(a, b):
    return jnp.concatenate([a, b], axis=-1)


def gelu(x):
    inner = (x + 0.044715 * x * x * x) * math.sqrt(2.0 / math.pi)
    return 0.5 * x * (1.0 + jnp.tanh(inner))


def slot(owner, me, devs):
    return lax.rem(owner - me + devs, devs)


def put_modes(kept, outs, at, held, me):
    devs = len(outs[0])
    for k, (re, im) in enumerate(kept):
        r = slot(k // 2, me, devs)
        held[r, k % 2, 0] = re
        held[r, k % 2, 1] = im
    for kk in range(2):
        for r in range(devs):
            for p in range(2):
                outs[kk][r][p, 0, 0, at, :] = held[r, kk, p]


def loop_tiles(width, body):
    @pl.loop(0, width // SUB)
    def _(t):
        body(pl.ds(pl.multiple_of(t * SUB, SUB), SUB))


def first_kernel(devs, pos_ref, v_ref, pair_ref, *rest):
    outs, held = (rest[:devs], rest[devs:2 * devs]), rest[-1]
    depth, width = v_ref.shape[2], v_ref.shape[3]

    def body(at):
        tiles = []
        for z in range(depth):
            tile = join(v_ref[0, 0, z, at, :], v_ref[0, 1, z, at, :])
            pair_ref[0, 0, z, at, :] = tile
            tiles.append(tile)
        put_modes(real_forward(tiles), outs, at, held, pos_ref[1])

    loop_tiles(width, body)


def point_kernel(v_ref, w_ref, b_ref, o_ref):
    depth = v_ref.shape[2]
    group = 8

    @pl.loop(0, depth // group)
    def _(g):
        cols = jnp.concatenate([v_ref[0, 0, g * group + i] for i in range(group)], axis=-1)
        out = jnp.dot(w_ref[...], cols, precision=EXACT, preferred_element_type=jnp.float32)
        for i in range(group):
            o_ref[0, 0, g * group + i] = out[:, i * 2 * HALF:(i + 1) * 2 * HALF] + b_ref[...]


def forward_x_kernel(x_devs, pos_ref, *refs):
    ins, held = refs[:x_devs], refs[-1]
    outs = refs[x_devs:-1]
    _, x_loc, _, width, _ = ins[0].shape
    size = x_devs * x_loc
    kept = size // 2
    devs, per = len(outs), outs[0].shape[0]

    def load(x):
        ref = ins[(x_devs - x // x_loc) % x_devs]
        return lambda at: (ref[0, x % x_loc, 0, at, :], ref[1, x % x_loc, 0, at, :])

    def body(at):
        even = fft([load(x)(at) for x in range(0, size, 2)], -1.0)
        odd = fft([load(x)(at) for x in range(1, size, 2)], -1.0)
        for q in range(kept):
            angle = -2.0 * math.pi * freq(q, kept, size) / size
            re, im = add(even[q], turn(odd[q], math.cos(angle), math.sin(angle)))
            r = slot(q // per, pos_ref[0], devs)
            held[r, q % per, 0] = re
            held[r, q % per, 1] = im
        for r in range(devs):
            for i in range(per):
                for p in range(2):
                    outs[r][i, p, 0, at, :] = held[r, i, p]

    loop_tiles(width, body)


def inverse_x_kernel(devs, pos_ref, *refs):
    ins, held = refs[:devs], refs[-1]
    outs = refs[devs:-1]
    per = ins[0].shape[0]
    _, x_loc, _, width, _ = outs[0].shape
    size = len(outs) * x_loc
    kept = size // 2

    def body(at):
        for r in range(devs):
            owner = slot(pos_ref[0], r, devs)
            for i in range(per):
                for p in range(2):
                    held[owner, i, p] = ins[r][i, p, 0, at, :]
        modes = [(held[q // per, q % per, 0], held[q // per, q % per, 1]) for q in range(kept)]
        for odd in range(2):
            twisted = []
            for q in range(kept):
                angle = 2.0 * math.pi * odd * freq(q, kept, size) / size
                twisted.append(turn(modes[q], math.cos(angle), math.sin(angle)))
            for i, (re, im) in enumerate(fft(twisted, 1.0)):
                x = 2 * i + odd
                outs[x // x_loc][0, x % x_loc, 0, at, :] = re
                outs[x // x_loc][1, x % x_loc, 0, at, :] = im

    loop_tiles(width, body)


def mix_kernel(devs, parts, pos_ref, *refs):
    count = devs * parts
    ins, (re_ref, im_ref), outs = refs[:count], refs[count:count + 2], refs[count + 2:2 * count + 2]
    spec_ref, mixed_ref = refs[2 * count + 2:]
    _, _, part, width, lanes = ins[0].shape
    kept = count * part
    size = 2 * kept
    low = lax.broadcasted_iota(jnp.int32, (SUB, lanes), 1) < HALF
    low_wide = lax.broadcasted_iota(jnp.int32, (width, lanes), 1) < HALF

    def place(j):
        ahead, pair = divmod(j, parts * part)
        return ahead, pair // part, pair % part

    def forward(at):
        values = []
        for j in range(kept):
            ahead, h, i = place(j)
            ref = ins[h * devs + (devs - ahead) % devs]
            values.append((ref[0, 0, i, at, :], ref[0, 1, i, at, :]))
        modes = fft(values, -1.0)
        for q in range(kept):
            angle = -2.0 * math.pi * freq(q, kept, size) / size
            re, im = modes[q]
            far_re, far_im = turn((re, im), math.cos(angle), math.sin(angle))
            near = jnp.where(low, re, far_im)
            far = jnp.where(low, im, far_re)
            spec_ref[q, at, :] = near + pltpu.roll(far, HALF, 1)

    loop_tiles(width, forward)
    flip = jnp.where(low_wide, -1.0, 1.0)
    for q in range(kept):
        weight = jnp.concatenate([re_ref[0, 0, q, 0], im_ref[0, 0, q, 0]], axis=-1)
        out = lax.dot_general(weight, spec_ref[q], (((0,), (0,)), ((), ())), precision=EXACT, preferred_element_type=jnp.float32)
        mixed_ref[q] = out[:width] + pltpu.roll(out[width:], HALF, 1) * flip

    def inverse(at):
        twisted = []
        for q in range(kept):
            both = mixed_ref[q, at, :]
            swap = pltpu.roll(both, HALF, 1)
            re, im = jnp.where(low, both, swap), jnp.where(low, swap, both)
            angle = 2.0 * math.pi * freq(q, kept, size) / size
            far_re, far_im = turn((re, im), math.cos(angle), math.sin(angle))
            twisted.append((jnp.where(low, re, far_re), jnp.where(low, im, far_im)))
        for j, (re, im) in enumerate(fft(twisted, 1.0)):
            ahead, h, i = place(j)
            outs[h * devs + ahead][0, 0, i, at, :] = re
            outs[h * devs + ahead][0, 1, i, at, :] = im

    loop_tiles(width, inverse)


def last_kernel(devs, scale, more, pos_ref, *refs):
    ins, p_ref, rest = (refs[:devs], refs[devs:2 * devs]), refs[2 * devs], refs[2 * devs + 1:]
    got, held = rest[-2:]
    depth, width = p_ref.shape[2], p_ref.shape[3]
    me = pos_ref[1]

    def body(at):
        for r in range(devs):
            owner = slot(me, r, devs)
            for kk in range(2):
                for p in range(2):
                    got[owner, kk, p] = ins[kk][r][p, 0, 0, at, :]
        spectral = real_inverse([(got[k // 2, k % 2, 0], got[k // 2, k % 2, 1]) for k in range(2 * devs)], scale)
        fresh = []
        for z in range(depth):
            tile = gelu(spectral[z] + p_ref[0, 0, z, at, :])
            if more:
                rest[0][0, 0, z, at, :] = tile
                fresh.append(tile)
            else:
                rest[-3][0, 0, z, at, :] = tile[:, :HALF]
                rest[-3][0, 1, z, at, :] = tile[:, HALF:]
        if more:
            put_modes(real_forward(fresh), (rest[1:devs + 1], rest[devs + 1:2 * devs + 1]), at, held, me)

    loop_tiles(width, body)


PARTS = 2


def cost(us):
    return pl.CostEstimate(flops=int(us * FLOPS_PER_US), bytes_accessed=1048576, transcendentals=0)


FLOPS_PER_US = 30000000


def solution(mesh):
    row_devs = mesh.shape['ys']
    col_devs = mesh.shape['xs']

    def local_layers(field, spec_real, spec_imag, mix_weight, bias):
        batch, x_loc, y_loc, grid_z, width = field.shape
        modes = spec_real.shape[3]
        layers = spec_real.shape[0]
        lanes = 2 * batch
        pairs = y_loc // 2
        part = pairs // PARTS
        per = 2 * modes // row_devs
        scale = 1.0 / (x_loc * col_devs * y_loc * row_devs * grid_z)
        shape = lambda *dims: jax.ShapeDtypeStruct(dims, jnp.float32)
        scratch = lambda *dims: pltpu.VMEM(dims, jnp.float32)
        wave = (2, x_loc, part, width, lanes)
        freqs = (per, 2, part, width, lanes)
        cells = (x_loc, part, grid_z, width, lanes)
        wave_cell = pl.BlockSpec((2, 1, 1, width, lanes), lambda x, y, pos: (0, x, y, 0, 0))
        wave_row = pl.BlockSpec((2, x_loc, 1, width, lanes), lambda y, pos: (0, 0, y, 0, 0))
        freq_row = pl.BlockSpec((per, 2, 1, width, lanes), lambda y, pos: (0, 0, y, 0, 0))
        freq_cell = pl.BlockSpec((1, 2, part, width, lanes), lambda q, pos: (q, 0, 0, 0, 0))
        cell = pl.BlockSpec((1, 1, grid_z, width, lanes), lambda x, y, pos: (x, y, 0, 0, 0))
        loose = lambda h: pl.BlockSpec((1, 2, grid_z, width, batch), lambda x, y, pos: (x, y + h * part, 0, 0, 0))
        position = jnp.stack([lax.axis_index('ys'), lax.axis_index('xs')]).astype(jnp.int32)

        def call(body, us, grid, ins, outs, shapes, scratches, *operands, alias=None):
            spec = pltpu.PrefetchScalarGridSpec(num_scalar_prefetch=1, grid=grid, in_specs=ins, out_specs=outs, scratch_shapes=scratches)
            return pl.pallas_call(body, grid_spec=spec, out_shape=shapes, cost_estimate=cost(us), input_output_aliases=alias or {},
                                  compiler_params=pltpu.CompilerParams(dimension_semantics=('arbitrary',) * len(grid)))(position, *operands)

        def swap(arrays, axis):
            devs = len(arrays)
            return [arrays[0]] + [lax.ppermute(arrays[r], axis, [(i, (i + r) % devs) for i in range(devs)]) for r in range(1, devs)]

        def first(h, grid_field):
            out = call(functools.partial(first_kernel, col_devs), 18, (x_loc, part), [loose(h)], [cell] + [wave_cell] * (2 * col_devs),
                       [shape(*cells)] + [shape(*wave)] * (2 * col_devs), [scratch(col_devs, 2, 2, SUB, lanes)], grid_field)
            return out[0], [out[1:1 + col_devs], out[1 + col_devs:]]

        def forward_x(arrays):
            return call(functools.partial(forward_x_kernel, col_devs), 3, (part,), [wave_row] * col_devs, [freq_row] * row_devs,
                        [shape(*freqs)] * row_devs, [scratch(row_devs, per, 2, SUB, lanes)], *arrays)

        def inverse_x(arrays):
            return call(functools.partial(inverse_x_kernel, row_devs), 3, (part,), [freq_row] * row_devs, [wave_row] * col_devs,
                        [shape(*wave)] * col_devs, [scratch(row_devs, per, 2, SUB, lanes)], *arrays)

        def mix(layer, kk, arrays):
            weight = pl.BlockSpec((1, 1, 2 * modes, 1, width, width), lambda q, pos: (layer, pos[0] * per + q, 0, 2 * pos[1] + kk, 0, 0))
            count = row_devs * PARTS
            out = call(functools.partial(mix_kernel, row_devs, PARTS), 11, (per,), [freq_cell] * count + [weight] * 2, [freq_cell] * count,
                       [shape(*freqs)] * count, [scratch(2 * modes, width, lanes)] * 2, *arrays, spec_real, spec_imag)
            return [list(out[h * row_devs:(h + 1) * row_devs]) for h in range(PARTS)]

        def point(layer, value, half, target):
            body = lambda pos_ref, *refs: point_kernel(*refs[:3], refs[-1])
            whole = lambda *dims: pl.BlockSpec(dims, lambda x, y, pos: (0, 0))
            rows = x_loc // 2
            place = pl.BlockSpec((1, 1, grid_z, width, lanes), lambda x, y, pos: (x + half * rows, y, 0, 0, 0))
            ins = [place, whole(width, width), whole(width, lanes)]
            operands = [value, mix_weight[layer].T, jnp.broadcast_to(bias[layer][:, None], (width, lanes))]
            if target is None:
                return call(body, 10, (rows, part), ins, place, shape(*cells), [], *operands)
            return call(body, 10, (rows, part), ins + [pl.BlockSpec(memory_space=pl.ANY)], place, shape(*cells), [], *operands, target, alias={4: 0})

        def last(h, more, arrays, local, target):
            scratches = [scratch(col_devs, 2, 2, SUB, lanes)] * 2
            body = functools.partial(last_kernel, col_devs, scale, more)
            ins = [wave_cell] * (2 * col_devs) + [cell]
            if more:
                out = call(body, 17, (x_loc, part), ins, [cell] + [wave_cell] * (2 * col_devs), [shape(*cells)] + [shape(*wave)] * (2 * col_devs), scratches, *arrays, local)
                return out[0], [out[1:1 + col_devs], out[1 + col_devs:]]
            whole = shape(x_loc, y_loc, grid_z, width, batch)
            if target is None:
                return call(body, 18, (x_loc, part), ins, loose(h), whole, scratches, *arrays, local)
            return call(body, 18, (x_loc, part), ins + [pl.BlockSpec(memory_space=pl.ANY)], loose(h), whole, scratches, *arrays, local, target, alias={len(ins) + 1: 0})

        grid_field = field.transpose(1, 2, 3, 4, 0)
        values, waves = zip(*[first(h, grid_field) for h in range(PARTS)])
        target = None

        def after(done, arrays):
            done[0], arrays[0] = lax.optimization_barrier((done[0], arrays[0]))

        order = [(kk, h) for kk in range(2) for h in range(PARTS)]

        def run_layer(layer, values, waves, target):
            along, previous = {}, None
            local = [None] * PARTS

            def piece(h, half, done, arrays):
                done[0], values[h] = lax.optimization_barrier((done[0], values[h]))
                local[h] = point(layer, values[h], half, local[h])
                local[h], arrays[0] = lax.optimization_barrier((local[h], arrays[0]))

            for n, (kk, h) in enumerate(order):
                arrays = swap(waves[h][kk], 'xs')
                if n == 2:
                    piece(0, 0, previous, arrays)
                elif n:
                    after(previous, arrays)
                previous = list(forward_x(arrays))
                along[kk, h] = previous
            mixed, previous = [], along[order[-1]]
            for kk in range(2):
                arrays = sum([swap(along[kk, h], 'ys') for h in range(PARTS)], [])
                if kk:
                    piece(0, 1, previous, arrays)
                mixed.append(mix(layer, kk, arrays))
                previous = mixed[-1][0]
            back = [[None] * PARTS for _ in range(2)]
            for n, (kk, h) in enumerate(order):
                arrays = swap(mixed[kk][h], 'ys')
                if n == 2:
                    piece(1, 0, previous, arrays)
                else:
                    after(previous if n else mixed[1][1], arrays)
                previous = list(inverse_x(arrays))
                back[kk][h] = previous
            back = [[swap(back[kk][h], 'xs') for h in range(PARTS)] for kk in range(2)]
            piece(1, 1, back[1][1], back[0][0])
            more = layer + 1 < layers
            fresh = []
            for h in range(PARTS):
                target = last(h, more, list(back[0][h]) + list(back[1][h]), local[h], None if more else target)
                fresh.append(target)
            if more:
                values, waves = zip(*fresh)
                target = None
            return values, waves, target

        for layer in range(layers):
            values, waves, target = run_layer(layer, list(values), waves, target)
        return target.transpose(4, 0, 1, 2, 3)


    field_spec = P('data', 'xs', 'ys', None, None)
    return jax.shard_map(local_layers, mesh=mesh, in_specs=(field_spec, P(), P(), P(), P()), out_specs=field_spec, check_vma=False)
```
